768 devices in a mesh: grp: 32 (over y, x), wide: 24 (over z, core).
Axes of the slice: x: 4, y: 8, z: 12, core: 2. Of those that a mesh axis runs over, the one named last changes fastest.
Arguments:
- gradient: bfloat16 [32, 24, 96, 4096], P('grp', 'wide'), may hold values from -6 to 6
- residual: float32 [32, 24, 96, 4096], P('grp', 'wide'), may hold values from -4 to 4
- selected: int32 [32, 24, 24, 32], P('grp', 'wide'), may hold values from 0 to 127, as said below
- counts: int32 [32, 24, 24], P('grp', 'wide'), may hold values from 1 to 32, as said below
Outputs:
- update: float32 [24, 4, 4096], P('wide')
- new_residual: float32 [32, 24, 96, 4096], P('grp', 'wide')
The draws below stay inside these ranges and needn't reach their ends.
Inputs may be any that keep to these rules, and one draw needn't show every extreme that they name: `selected`: for each device and shard, 32 distinct block numbers of that shard; entries at or past the count are ignored. `counts`: one shard has 32 on every device; every device has at most one other shard at 32, the rest at most 16.
All inputs are finite; a program needn't handle non-finite values.
Results may differ from the reference program's by a relative error of at most 0.0003.
Values sent between devices are 32-bit elements; how exact they have to be, the bound alone decides.
A program may use at most 32 MiB of HBM per device.

```python
import jax
import jax.numpy as jnp

D = 4096
BW = 128
OWN_ROWS = 4
W_ROWS = 96
OWN_BLK = 128
KMAX = 32
N_GRP = 32
N_WIDE = 24


def draw_selected(key, part):
    scores = jax.random.randint(key, (N_GRP, N_WIDE, N_WIDE, OWN_BLK), 0, 1 << 20)
    scores = scores * OWN_BLK + jnp.arange(OWN_BLK, dtype=jnp.int32)
    order = jnp.argsort(scores, axis=-1)
    return order[..., :KMAX].astype(jnp.int32)


def draw_counts(key, part):
    first, second, third = jax.random.split(jax.random.fold_in(key, 7), 3)
    base = jax.random.randint(first, (N_GRP, N_WIDE, N_WIDE), max(1, KMAX // 8), KMAX // 2 + 1)
    common = jax.random.randint(second, (), 0, N_WIDE)
    personal = jax.random.randint(third, (N_GRP, N_WIDE, 1), 0, N_WIDE)
    shard = jnp.arange(N_WIDE, dtype=jnp.int32)[None, None, :]
    hottest = jnp.logical_or(shard == common, shard == personal)
    return jnp.where(hottest, KMAX, base).astype(jnp.int32)


def levels(key, dims, cuts, least, high):
    level, own = 1.0, jax.random.fold_in(key, 6)
    for dim, shards_of in cuts:
        steps = jnp.exp(jax.random.uniform(jax.random.fold_in(own, dim), (shards_of,), jnp.float32, least / len(cuts), high / len(cuts)))
        level = level * jnp.repeat(steps, dims[dim] // shards_of).reshape([-1 if axis == dim else 1 for axis in range(len(dims))])
    return level


def gaussian(rng, extent, deviation, limit, pieces=(), held_as=jnp.bfloat16):
    factor_of = levels(rng, extent, pieces, -0.22, 0.18) if pieces else 1.0
    result = jax.random.normal(rng, extent, jnp.float32) * deviation * factor_of
    return jnp.minimum(jnp.maximum(result, -limit), limit).astype(held_as)


def setup_inputs(seed: int = 0) -> dict:
    seeds = jax.random.split(jax.random.key(seed), 5)
    return {
        "gradient": gaussian(seeds[0], (N_GRP, N_WIDE, W_ROWS, D), 1.0, 6.0, ((0, 32), (1, 24))),
        "residual": gaussian(seeds[1], (N_GRP, N_WIDE, W_ROWS, D), 0.5, 4.0, ((0, 32), (1, 24)), jnp.float32),
        "selected": draw_selected(jax.random.fold_in(seeds[4], 71), 0),
        "counts": draw_counts(jax.random.fold_in(seeds[4], 71), 0),
    }


def reference(gradient, residual, selected, counts):
    accumulated = gradient.astype(jnp.float32) + residual
    blocks = accumulated.reshape(N_GRP, N_WIDE, N_WIDE, OWN_BLK, BW)
    slot_ids = jnp.arange(KMAX, dtype=jnp.int32)
    valid = (slot_ids[None, None, None, :] < counts[..., None]).astype(jnp.float32)
    block_ids = jnp.arange(OWN_BLK, dtype=jnp.int32)
    hits = (selected[..., None] == block_ids).astype(jnp.float32)
    mask = jnp.sum(hits * valid[..., None], axis=3)
    new_residual = (blocks * (1.0 - mask[..., None])).reshape(N_GRP, N_WIDE, W_ROWS, D)
    total = jnp.sum(blocks * mask[..., None], axis=(0, 1))
    update = (total / N_GRP).reshape(N_WIDE, OWN_ROWS, D)
    return update, new_residual
```

```python
import jax
import jax.numpy as jnp
from jax import lax
from jax.experimental import pallas as pl
from jax.experimental.pallas import tpu as pltpu
from jax.sharding import PartitionSpec as P

MESH = pl.DeviceIdType.MESH
NX, NY, NZ, NC = 4, 8, 12, 2
CHUNKS = 3
F32, BF16, I32 = jnp.float32, jnp.bfloat16, jnp.int32


def ring(d, n):
    return min(d % n, (-d) % n)


XC = sorted(
    [(dx, dc) for dx in range(NX) for dc in range(NC) if dx or dc],
    key=lambda o: -(2 * ring(o[0], NX) + o[1]),
)
YS = sorted(range(1, NY), key=lambda d: -ring(d, NY))
GS = sorted(
    [(dx, dy) for dx in range(NX) for dy in range(NY) if dx or dy],
    key=lambda o: -(ring(o[0], NX) + ring(o[1], NY)),
)


def halves(v):
    hi = v.astype(BF16)
    lo = (v - hi.astype(F32)).astype(BF16)
    return jnp.concatenate([hi, lo], axis=1)


def joined(v):
    return v[:, :128] + v[:, 128:]


def kernel(
    g_hbm, r_hbm, sel_ref, cnt_ref, upd_ref, nr_hbm,
    gv, rv, nrv, xsend, xrecv, idsend, idrecv, ysend, yrecv, zsend, zrecv, fin, gbuf,
    gsem, rsem, nsem, xs, xr, ids_s, ids_r, ys, yr, zs, zr, as_, ar,
):
    gi = lax.axis_index("grp")
    wi = lax.axis_index("wide")
    x, y = lax.rem(gi, NX), lax.div(gi, NX)
    z, c = lax.div(wi, NC), lax.rem(wi, NC)

    def dev(x_, y_, z_, c_):
        return (y_ * NX + x_, z_ * NC + c_)

    def mod(a, n):
        return lax.rem(a + n, n)

    loads = []
    for j in range(CHUNKS):
        rows = pl.ds(32 * j, 32)
        a = pltpu.make_async_copy(g_hbm.at[0, 0, rows], gv.at[rows], gsem.at[j])
        b = pltpu.make_async_copy(r_hbm.at[0, 0, rows], rv.at[rows], rsem.at[j])
        a.start()
        b.start()
        loads.append((a, b))

    barrier = pltpu.get_barrier_semaphore()
    zx = lax.rem(z, NX)
    for dz in sorted(range(1, NZ), key=lambda d: -ring(d, NZ)):
        pl.semaphore_signal(barrier, inc=1, device_id=dev(zx, y, mod(z + dz, NZ), c), device_id_type=MESH)
    for dx, dy in GS:
        pl.semaphore_signal(
            barrier, inc=1, device_id=dev(mod(x + dx, NX), mod(y + dy, NY), z, c), device_id_type=MESH
        )
    for dx in range(NX):
        pl.semaphore_signal(
            barrier, inc=1, device_id=dev(mod(x + dx, NX), y, z, mod(c + 1, NC)), device_id_type=MESH
        )

    sel = sel_ref[0, 0]
    eye = lax.broadcasted_iota(I32, (24, 24), 0) == lax.broadcasted_iota(I32, (24, 24), 1)
    used = jnp.sum(
        jnp.where(eye, jnp.broadcast_to(cnt_ref[0], (24, 24)).astype(F32), 0.0), axis=1, keepdims=True
    ).astype(I32)
    valid = lax.broadcasted_iota(I32, (24, 32), 1) < used
    low, high = jnp.bitwise_and(sel, 31), jnp.right_shift(sel, 5)
    target = jnp.where(valid, low * 4 + high, 512)
    odd = jnp.bitwise_and(lax.broadcasted_iota(I32, (24, 32), 0), 1)
    source = jnp.where(valid, low * 8 + high + 4 * odd, 512)
    target4 = jnp.concatenate([target] * 4, axis=1)
    source4 = jnp.concatenate([source] * 4, axis=1)
    for j in range(CHUNKS):
        for d in range(8):
            idsend[j, d] = target4[8 * j + d : 8 * j + d + 1]
    source_t = jnp.transpose(source4.astype(F32)).astype(I32)
    lane128 = lax.broadcasted_iota(I32, (1, 128), 1)
    lane256 = lax.broadcasted_iota(I32, (64, 256), 1)
    sub256 = lax.broadcasted_iota(I32, (256, 128), 0)
    ones = jnp.ones((128, 128), BF16)

    owner_class = jnp.bitwise_and(z - x, 3)
    same = lax.div(4 - owner_class, 4)
    pl.semaphore_wait(barrier, 47 - 4 * same)

    mine = 2 * x + c
    pending = []
    idcopies = []
    for n, (dx, dc) in enumerate(XC):
        tx, tc = mod(x + dx, NX), mod(c + dc, NC)
        cp = pltpu.make_async_remote_copy(
            src_ref=idsend.at[:, 2 * tx + tc], dst_ref=idrecv.at[n + 1],
            send_sem=ids_s.at[n], recv_sem=ids_r.at[n],
            device_id=dev(tx, y, z, tc), device_id_type=MESH,
        )
        cp.start()
        idcopies.append(cp)
    idrecv[0] = idsend[:, mine]

    xcopies = []
    writes = []
    for j in range(CHUNKS):
        loads[j][0].wait()
        loads[j][1].wait()
        for p in range(4):
            s = 8 * j + 2 * p
            top = 32 * j + 8 * p
            blocks = []
            for q in range(32):
                lanes = slice(128 * q, 128 * (q + 1))
                blocks.append(gv[top : top + 8, lanes].astype(F32) + rv[top : top + 8, lanes])
            data = jnp.concatenate(blocks, axis=0)
            ids = jnp.concatenate(
                [
                    jnp.broadcast_to(source_t[:32, s : s + 1], (32, 256)),
                    jnp.broadcast_to(source_t[:32, s + 1 : s + 2], (32, 256)),
                ],
                axis=0,
            )
            pick = jnp.where(ids == lane256, 1.0, 0.0).astype(BF16)
            got = joined(jnp.dot(pick, halves(data), preferred_element_type=F32))
            xsend[j, 2 * p] = got[:32]
            xsend[j, 2 * p + 1] = got[32:]
            row = jnp.where(lane128 < 32, source4[s : s + 1], source4[s + 1 : s + 2])
            hit = jnp.where(jnp.broadcast_to(row, (256, 128)) == sub256, 1.0, 0.0).astype(BF16)
            mask = jnp.dot(hit, ones, preferred_element_type=F32)
            kept = jnp.where(mask > 0.5, 0.0, data)
            for q in range(32):
                nrv[top : top + 8, 128 * q : 128 * (q + 1)] = kept[8 * q : 8 * q + 8]
        copies = []
        for n, (dx, dc) in enumerate(XC):
            tx, tc = mod(x + dx, NX), mod(c + dc, NC)
            cp = pltpu.make_async_remote_copy(
                src_ref=xsend.at[j, 2 * tx + tc], dst_ref=xrecv.at[j, n + 1],
                send_sem=xs.at[j, n], recv_sem=xr.at[j, n],
                device_id=dev(tx, y, z, tc), device_id_type=MESH,
            )
            cp.start()
            copies.append(cp)
        xrecv[j, 0] = xsend[j, mine]
        xcopies.append(copies)
        rows = pl.ds(32 * j, 32)
        w = pltpu.make_async_copy(nrv.at[rows], nr_hbm.at[0, 0, rows], nsem.at[j])
        w.start()
        writes.append(w)

    for cp in idcopies:
        cp.wait_recv()
    quarter = jnp.right_shift(lane128, 5)
    sub128 = lax.broadcasted_iota(I32, (128, 256), 0)
    ycopies = []
    for j in range(CHUNKS):
        for cp in xcopies[j]:
            cp.wait_recv()
        parts = []
        for h in range(2):
            row = idrecv[4 * h, j]
            for q in range(1, 4):
                row = jnp.where(quarter == q, idrecv[4 * h + q, j], row)
            parts.append(row)
        ids = jnp.broadcast_to(jnp.concatenate(parts, axis=1), (128, 256))
        put = jnp.where(ids == sub128, 1.0, 0.0).astype(BF16)
        arrived = xrecv[j].reshape(256, 128)
        ysend[j] = joined(jnp.dot(put, halves(arrived), preferred_element_type=F32)).reshape(8, 16, 128)
        copies = []
        for n, dy in enumerate(YS):
            ty = mod(y + dy, NY)
            cp = pltpu.make_async_remote_copy(
                src_ref=ysend.at[j, ty], dst_ref=yrecv.at[j, n],
                send_sem=ys.at[j, n], recv_sem=yr.at[j, n],
                device_id=dev(x, ty, z, c), device_id_type=MESH,
            )
            cp.start()
            copies.append(cp)
        ycopies.append(copies)

    zcopies = []
    for j in range(CHUNKS):
        for cp in ycopies[j]:
            cp.wait_recv()
        total = ysend[j, y]
        for n in range(NY - 1):
            total = total + yrecv[j, n]
        for q in range(4):
            zsend[j, q] = total[4 * q : 4 * q + 4]
        tz = 4 * j + x
        for dq in (2, 1, 3):
            tq = mod(x + dq, NX)
            cp = pltpu.make_async_remote_copy(
                src_ref=zsend.at[j, tq], dst_ref=zrecv.at[z],
                send_sem=zs.at[j, dq], recv_sem=zr.at[z],
                device_id=dev(tq, y, tz, c), device_id_type=MESH,
            )
            cp.start()
            zcopies.append(cp)

        def same_x(j=j, tz=tz):
            return pltpu.make_async_remote_copy(
                src_ref=zsend.at[j, x], dst_ref=zrecv.at[z],
                send_sem=zs.at[j, 0], recv_sem=zr.at[z],
                device_id=dev(x, y, tz, c), device_id_type=MESH,
            )

        @pl.when(tz != z)
        def _():
            same_x().start()

        @pl.when(tz == z)
        def _():
            zrecv[z] = zsend[j, x]

    for s in range(NZ):
        @pl.when(jnp.logical_or(zx != x, z != s))
        def _():
            pltpu.make_async_remote_copy(
                src_ref=zsend.at[0, 0], dst_ref=zrecv.at[s],
                send_sem=zs.at[0, 0], recv_sem=zr.at[s],
                device_id=dev(x, y, z, 1 - c), device_id_type=MESH,
            ).wait_recv()

    result = zrecv[0]
    for s in range(1, NZ):
        result = result + zrecv[s]
    result = result * (1.0 / 32.0)
    fin[...] = result
    gcopies = []
    for n, (dx, dy) in enumerate(GS):
        cp = pltpu.make_async_remote_copy(
            src_ref=fin, dst_ref=gbuf.at[gi],
            send_sem=as_.at[n], recv_sem=ar.at[gi],
            device_id=dev(mod(x + dx, NX), mod(y + dy, NY), z, c), device_id_type=MESH,
        )
        cp.start()
        gcopies.append(cp)
    gbuf[gi] = result

    for cp in idcopies:
        cp.wait_send()
    for copies in xcopies + ycopies:
        for cp in copies:
            cp.wait_send()
    for cp in zcopies:
        cp.wait_send()
    for j in range(CHUNKS):
        tz = 4 * j + x

        @pl.when(tz != z)
        def _():
            pltpu.make_async_remote_copy(
                src_ref=zsend.at[j, x], dst_ref=zrecv.at[z],
                send_sem=zs.at[j, 0], recv_sem=zr.at[z],
                device_id=dev(x, y, tz, c), device_id_type=MESH,
            ).wait_send()
    for w in writes:
        w.wait()
    for n, (dx, dy) in enumerate(GS):
        sg = mod(y - dy, NY) * NX + mod(x - dx, NX)
        pltpu.make_async_remote_copy(
            src_ref=fin, dst_ref=gbuf.at[sg],
            send_sem=as_.at[n], recv_sem=ar.at[sg],
            device_id=dev(mod(x + dx, NX), mod(y + dy, NY), z, c), device_id_type=MESH,
        ).wait_recv()
    for cp in gcopies:
        cp.wait_send()
    for p in range(32):
        upd_ref[0, :, 128 * p : 128 * (p + 1)] = gbuf[p]


def body(gradient, residual, selected, counts):
    dma = pltpu.SemaphoreType.DMA
    vmem = pl.BlockSpec(memory_space=pltpu.VMEM)
    anyspace = pl.BlockSpec(memory_space=pl.ANY)
    return pl.pallas_call(
        kernel,
        name="owner_sums",
        out_shape=(
            jax.ShapeDtypeStruct((1, 4, 4096), F32),
            jax.ShapeDtypeStruct((1, 1, 96, 4096), F32),
        ),
        in_specs=[anyspace, anyspace, vmem, vmem],
        out_specs=(vmem, anyspace),
        scratch_shapes=[
            pltpu.VMEM((96, 4096), BF16),
            pltpu.VMEM((96, 4096), F32),
            pltpu.VMEM((96, 4096), F32),
            pltpu.VMEM((CHUNKS, 8, 32, 128), F32),
            pltpu.VMEM((CHUNKS, 8, 32, 128), F32),
            pltpu.VMEM((CHUNKS, 8, 1, 128), I32),
            pltpu.VMEM((8, CHUNKS, 1, 128), I32),
            pltpu.VMEM((CHUNKS, 8, 16, 128), F32),
            pltpu.VMEM((CHUNKS, 7, 16, 128), F32),
            pltpu.VMEM((CHUNKS, 4, 4, 128), F32),
            pltpu.VMEM((NZ, 4, 128), F32),
            pltpu.VMEM((4, 128), F32),
            pltpu.VMEM((32, 4, 128), F32),
            dma((CHUNKS,)), dma((CHUNKS,)), dma((CHUNKS,)),
            dma((CHUNKS, 7)), dma((CHUNKS, 7)),
            dma((7,)), dma((7,)),
            dma((CHUNKS, 7)), dma((CHUNKS, 7)),
            dma((CHUNKS, 4)), dma((NZ,)),
            dma((31,)), dma((32,)),
        ],
        compiler_params=pltpu.CompilerParams(collective_id=0, has_side_effects=True),
    )(gradient, residual, selected, counts)


def solution(mesh):
    return jax.shard_map(
        body,
        mesh=mesh,
        in_specs=(
            P("grp", "wide", None, None),
            P("grp", "wide", None, None),
            P("grp", "wide", None, None),
            P("grp", "wide", None),
        ),
        out_specs=(P("wide", None, None), P("grp", "wide", None, None)),
        check_vma=False,
    )
```

```python
import jax
import jax.numpy as jnp
from jax import lax
from jax.experimental import pallas as pl
from jax.experimental.pallas import tpu as pltpu
from jax.sharding import PartitionSpec as P

MESH = pl.DeviceIdType.MESH
NX, NY, NZ, NC = 4, 8, 12, 2
CHUNKS = 3
F32, BF16, I32 = jnp.float32, jnp.bfloat16, jnp.int32


def ring(d, n):
    return min(d % n, (-d) % n)


XC = sorted(
    [(dx, dc) for dx in range(NX) for dc in range(NC) if dx or dc],
    key=lambda o: -(2 * ring(o[0], NX) + o[1]),
)
YS = sorted(range(1, NY), key=lambda d: -ring(d, NY))
GS = sorted(
    [(dx, dy) for dx in range(NX) for dy in range(NY) if dx or dy],
    key=lambda o: -(ring(o[0], NX) + ring(o[1], NY)),
)


def halves(v):
    hi = v.astype(BF16)
    lo = (v - hi.astype(F32)).astype(BF16)
    return jnp.concatenate([hi, lo], axis=1)


def joined(v):
    return v[:, :128] + v[:, 128:]


def kernel(
    g_hbm, r_hbm, sel_hbm, cnt_hbm, upd_ref, nr_ref,
    sel_ref, cnt_ref, gv, rv, xsend, xrecv, idsend, idrecv, ysend, yrecv, zsend, zrecv, fin, gbuf,
    psem, gsem, rsem, xs, xr, ids_s, ids_r, ys, yr, zs, zr, as_, ar, near1, near2, near3,
):
    gi = lax.axis_index("grp")
    wi = lax.axis_index("wide")
    x, y = lax.rem(gi, NX), lax.div(gi, NX)
    z, c = lax.div(wi, NC), lax.rem(wi, NC)

    def dev(x_, y_, z_, c_):
        return (y_ * NX + x_, z_ * NC + c_)

    def mod(a, n):
        return lax.rem(a + n, n)

    picks = (
        pltpu.make_async_copy(sel_hbm, sel_ref, psem.at[0]),
        pltpu.make_async_copy(cnt_hbm, cnt_ref, psem.at[1]),
    )
    for cp in picks:
        cp.start()
    loads = []
    for j in range(CHUNKS):
        rows = pl.ds(32 * j, 32)
        a = pltpu.make_async_copy(g_hbm.at[0, 0, rows], gv.at[rows], gsem.at[j])
        b = pltpu.make_async_copy(r_hbm.at[0, 0, rows], rv.at[rows], rsem.at[j])
        a.start()
        b.start()
        loads.append((a, b))

    def signal(sem, x_, y_, z_, c_):
        pl.semaphore_signal(sem, inc=1, device_id=dev(x_, y_, z_, c_), device_id_type=MESH)

    barrier = pltpu.get_barrier_semaphore()
    for d in (1, NZ - 1):
        signal(barrier, x, y, mod(z + d, NZ), c)
    for d in (1, NY - 1):
        signal(barrier, x, mod(y + d, NY), z, c)
    for dx, dc in XC:
        signal(barrier, mod(x + dx, NX), y, z, mod(c + dc, NC))

    for cp in picks:
        cp.wait()
    sel = sel_ref[0, 0]
    eye = lax.broadcasted_iota(I32, (24, 24), 0) == lax.broadcasted_iota(I32, (24, 24), 1)
    used = jnp.sum(
        jnp.where(eye, jnp.broadcast_to(cnt_ref[0], (24, 24)).astype(F32), 0.0), axis=1, keepdims=True
    ).astype(I32)
    valid = lax.broadcasted_iota(I32, (24, 32), 1) < used
    low, high = jnp.bitwise_and(sel, 31), jnp.right_shift(sel, 5)
    target = jnp.where(valid, low * 4 + high, 512)
    odd = jnp.bitwise_and(lax.broadcasted_iota(I32, (24, 32), 0), 1)
    source = jnp.where(valid, low * 8 + high + 4 * odd, 512)
    target4 = jnp.concatenate([target] * 4, axis=1)
    source4 = jnp.concatenate([source] * 4, axis=1)
    for j in range(CHUNKS):
        for d in range(8):
            idsend[j, d] = target4[8 * j + d : 8 * j + d + 1]
    source_t = jnp.transpose(source4.astype(F32)).astype(I32)
    lane128 = lax.broadcasted_iota(I32, (1, 128), 1)
    lane256 = lax.broadcasted_iota(I32, (64, 256), 1)
    sub256 = lax.broadcasted_iota(I32, (256, 128), 0)
    ones = jnp.ones((128, 128), BF16)

    mine = 2 * x + c
    idcopies = []
    xcopies = []
    for j in range(CHUNKS):
        loads[j][0].wait()
        loads[j][1].wait()
        for p in range(4):
            s = 8 * j + 2 * p
            top = 32 * j + 8 * p
            blocks = []
            for q in range(32):
                lanes = slice(128 * q, 128 * (q + 1))
                blocks.append(gv[top : top + 8, lanes].astype(F32) + rv[top : top + 8, lanes])
            data = jnp.concatenate(blocks, axis=0)
            ids = jnp.concatenate(
                [
                    jnp.broadcast_to(source_t[:32, s : s + 1], (32, 256)),
                    jnp.broadcast_to(source_t[:32, s + 1 : s + 2], (32, 256)),
                ],
                axis=0,
            )
            pick = jnp.where(ids == lane256, 1.0, 0.0).astype(BF16)
            got = joined(jnp.dot(pick, halves(data), preferred_element_type=F32))
            xsend[j, 2 * p] = got[:32]
            xsend[j, 2 * p + 1] = got[32:]
            row = jnp.where(lane128 < 32, source4[s : s + 1], source4[s + 1 : s + 2])
            hit = jnp.where(jnp.broadcast_to(row, (256, 128)) == sub256, 1.0, 0.0).astype(BF16)
            mask = jnp.dot(hit, ones, preferred_element_type=F32)
            kept = jnp.where(mask > 0.5, 0.0, data)
            for q in range(32):
                nr_ref[0, 0, top : top + 8, 128 * q : 128 * (q + 1)] = kept[8 * q : 8 * q + 8]
        if j == 0:
            pl.semaphore_wait(barrier, 11)
            for d in (1, NZ - 1):
                signal(near1, x, y, mod(z + d, NZ), c)
            for d in (1, NY - 1):
                signal(near1, x, mod(y + d, NY), z, c)
            for n, (dx, dc) in enumerate(XC):
                tx, tc = mod(x + dx, NX), mod(c + dc, NC)
                cp = pltpu.make_async_remote_copy(
                    src_ref=idsend.at[:, 2 * tx + tc], dst_ref=idrecv.at[n + 1],
                    send_sem=ids_s.at[n], recv_sem=ids_r.at[n],
                    device_id=dev(tx, y, z, tc), device_id_type=MESH,
                )
                cp.start()
                idcopies.append(cp)
            idrecv[0] = idsend[:, mine]
        if j == 1:
            pl.semaphore_wait(near1, 4)
            for d in (2, NZ - 2):
                signal(near2, x, y, mod(z + d, NZ), c)
            for d in (2, NY - 2):
                signal(near2, x, mod(y + d, NY), z, c)
        copies = []
        for n, (dx, dc) in enumerate(XC):
            tx, tc = mod(x + dx, NX), mod(c + dc, NC)
            cp = pltpu.make_async_remote_copy(
                src_ref=xsend.at[j, 2 * tx + tc], dst_ref=xrecv.at[j, n + 1],
                send_sem=xs.at[j, n], recv_sem=xr.at[j, n],
                device_id=dev(tx, y, z, tc), device_id_type=MESH,
            )
            cp.start()
            copies.append(cp)
        xrecv[j, 0] = xsend[j, mine]
        xcopies.append(copies)

    pl.semaphore_wait(near2, 4)
    for d in (3, NZ - 3):
        signal(near3, x, y, mod(z + d, NZ), c)
    for cp in idcopies:
        cp.wait_recv()
    quarter = jnp.right_shift(lane128, 5)
    sub128 = lax.broadcasted_iota(I32, (128, 256), 0)
    ycopies = []
    for j in range(CHUNKS):
        for cp in xcopies[j]:
            cp.wait_recv()
        parts = []
        for h in range(2):
            row = idrecv[4 * h, j]
            for q in range(1, 4):
                row = jnp.where(quarter == q, idrecv[4 * h + q, j], row)
            parts.append(row)
        ids = jnp.broadcast_to(jnp.concatenate(parts, axis=1), (128, 256))
        put = jnp.where(ids == sub128, 1.0, 0.0).astype(BF16)
        arrived = xrecv[j].reshape(256, 128)
        ysend[j] = joined(jnp.dot(put, halves(arrived), preferred_element_type=F32)).reshape(8, 16, 128)
        copies = []
        for n, dy in enumerate(YS):
            ty = mod(y + dy, NY)
            cp = pltpu.make_async_remote_copy(
                src_ref=ysend.at[j, ty], dst_ref=yrecv.at[j, n],
                send_sem=ys.at[j, n], recv_sem=yr.at[j, n],
                device_id=dev(x, ty, z, c), device_id_type=MESH,
            )
            cp.start()
            copies.append(cp)
        ycopies.append(copies)

    pl.semaphore_wait(near3, 2)
    zx = lax.rem(z, NX)
    zcopies = []
    for j in range(CHUNKS):
        for cp in ycopies[j]:
            cp.wait_recv()
        total = ysend[j, y]
        for n in range(NY - 1):
            total = total + yrecv[j, n]
        for q in range(4):
            zsend[j, q] = total[4 * q : 4 * q + 4]
        tz = 4 * j + x
        for dq in (2, 1, 3):
            tq = mod(x + dq, NX)
            cp = pltpu.make_async_remote_copy(
                src_ref=zsend.at[j, tq], dst_ref=zrecv.at[z],
                send_sem=zs.at[j, dq], recv_sem=zr.at[z],
                device_id=dev(tq, y, tz, c), device_id_type=MESH,
            )
            cp.start()
            zcopies.append(cp)

        def same_x(j=j, tz=tz):
            return pltpu.make_async_remote_copy(
                src_ref=zsend.at[j, x], dst_ref=zrecv.at[z],
                send_sem=zs.at[j, 0], recv_sem=zr.at[z],
                device_id=dev(x, y, tz, c), device_id_type=MESH,
            )

        @pl.when(tz != z)
        def _():
            same_x().start()

        @pl.when(tz == z)
        def _():
            zrecv[z] = zsend[j, x]

    for s in range(NZ):
        @pl.when(jnp.logical_or(zx != x, z != s))
        def _():
            pltpu.make_async_remote_copy(
                src_ref=zsend.at[0, 0], dst_ref=zrecv.at[s],
                send_sem=zs.at[0, 0], recv_sem=zr.at[s],
                device_id=dev(x, y, z, 1 - c), device_id_type=MESH,
            ).wait_recv()

    result = zrecv[0]
    for s in range(1, NZ):
        result = result + zrecv[s]
    result = result * (1.0 / 32.0)
    fin[...] = result
    gcopies = []
    for n, (dx, dy) in enumerate(GS):
        cp = pltpu.make_async_remote_copy(
            src_ref=fin, dst_ref=gbuf.at[gi],
            send_sem=as_.at[n], recv_sem=ar.at[gi],
            device_id=dev(mod(x + dx, NX), mod(y + dy, NY), z, c), device_id_type=MESH,
        )
        cp.start()
        gcopies.append(cp)
    gbuf[gi] = result

    for cp in idcopies:
        cp.wait_send()
    for copies in xcopies + ycopies:
        for cp in copies:
            cp.wait_send()
    for cp in zcopies:
        cp.wait_send()
    for j in range(CHUNKS):
        tz = 4 * j + x

        @pl.when(tz != z)
        def _():
            pltpu.make_async_remote_copy(
                src_ref=zsend.at[j, x], dst_ref=zrecv.at[z],
                send_sem=zs.at[j, 0], recv_sem=zr.at[z],
                device_id=dev(x, y, tz, c), device_id_type=MESH,
            ).wait_send()
    for n, (dx, dy) in enumerate(GS):
        sg = mod(y - dy, NY) * NX + mod(x - dx, NX)
        pltpu.make_async_remote_copy(
            src_ref=fin, dst_ref=gbuf.at[sg],
            send_sem=as_.at[n], recv_sem=ar.at[sg],
            device_id=dev(mod(x + dx, NX), mod(y + dy, NY), z, c), device_id_type=MESH,
        ).wait_recv()
    for cp in gcopies:
        cp.wait_send()
    for p in range(32):
        upd_ref[0, :, 128 * p : 128 * (p + 1)] = gbuf[p]


def flush(upd_ref, nr_ref, upd_hbm, nr_hbm, sem):
    copies = [pltpu.make_async_copy(upd_ref, upd_hbm, sem.at[4])]
    for n in range(4):
        rows = pl.ds(24 * n, 24)
        copies.append(pltpu.make_async_copy(nr_ref.at[0, 0, rows], nr_hbm.at[0, 0, rows], sem.at[n]))
    for cp in copies:
        cp.start()
    for cp in copies:
        cp.wait()


def body(gradient, residual, selected, counts):
    dma = pltpu.SemaphoreType.DMA
    plain = pltpu.SemaphoreType.REGULAR
    vmem = pl.BlockSpec(memory_space=pltpu.VMEM)
    hbm = pl.BlockSpec(memory_space=pltpu.HBM)
    update, rest = pl.pallas_call(
        kernel,
        name="owner_sums",
        out_shape=(
            pltpu.VMEM((1, 4, 4096), F32),
            pltpu.VMEM((1, 1, 96, 4096), F32),
        ),
        in_specs=[hbm, hbm, hbm, hbm],
        out_specs=(vmem, vmem),
        scratch_shapes=[
            pltpu.VMEM((1, 1, 24, 32), I32),
            pltpu.VMEM((1, 1, 24), I32),
            pltpu.VMEM((96, 4096), BF16),
            pltpu.VMEM((96, 4096), F32),
            pltpu.VMEM((CHUNKS, 8, 32, 128), F32),
            pltpu.VMEM((CHUNKS, 8, 32, 128), F32),
            pltpu.VMEM((CHUNKS, 8, 1, 128), I32),
            pltpu.VMEM((8, CHUNKS, 1, 128), I32),
            pltpu.VMEM((CHUNKS, 8, 16, 128), F32),
            pltpu.VMEM((CHUNKS, 7, 16, 128), F32),
            pltpu.VMEM((CHUNKS, 4, 4, 128), F32),
            pltpu.VMEM((NZ, 4, 128), F32),
            pltpu.VMEM((4, 128), F32),
            pltpu.VMEM((32, 4, 128), F32),
            dma((2,)), dma((CHUNKS,)), dma((CHUNKS,)),
            dma((CHUNKS, 7)), dma((CHUNKS, 7)),
            dma((7,)), dma((7,)),
            dma((CHUNKS, 7)), dma((CHUNKS, 7)),
            dma((CHUNKS, 4)), dma((NZ,)),
            dma((31,)), dma((32,)),
            plain, plain, plain,
        ],
        compiler_params=pltpu.CompilerParams(collective_id=0, has_side_effects=True, vmem_limit_bytes=62 << 20),
    )(gradient, residual, selected, counts)
    return pl.pallas_call(
        flush,
        name="write_results",
        out_shape=(
            jax.ShapeDtypeStruct((1, 4, 4096), F32),
            jax.ShapeDtypeStruct((1, 1, 96, 4096), F32),
        ),
        in_specs=[vmem, vmem],
        out_specs=(hbm, hbm),
        scratch_shapes=[dma((5,))],
        compiler_params=pltpu.CompilerParams(vmem_limit_bytes=1 << 20),
    )(update, rest)


def solution(mesh):
    return jax.shard_map(
        body,
        mesh=mesh,
        in_specs=(
            P("grp", "wide", None, None),
            P("grp", "wide", None, None),
            P("grp", "wide", None, None),
            P("grp", "wide", None),
        ),
        out_specs=(P("wide", None, None), P("grp", "wide", None, None)),
        check_vma=False,
    )
```

```python
import jax
import jax.numpy as jnp
from jax import lax
from jax.experimental import pallas as pl
from jax.experimental.pallas import tpu as pltpu
from jax.sharding import PartitionSpec as P

MESH = pl.DeviceIdType.MESH
NX, NY, NZ, NC = 4, 8, 12, 2
CHUNKS = 3
F32, BF16, I32 = jnp.float32, jnp.bfloat16, jnp.int32


def ring(d, n):
    return min(d % n, (-d) % n)


XC = sorted(
    [(dx, dc) for dx in range(NX) for dc in range(NC) if dx or dc],
    key=lambda o: -(2 * ring(o[0], NX) + o[1]),
)
YS = sorted(range(1, NY), key=lambda d: -ring(d, NY))
GS = sorted(
    [(dx, dy) for dx in range(NX) for dy in range(NY) if dx or dy],
    key=lambda o: -(ring(o[0], NX) + ring(o[1], NY)),
)


def halves(v):
    hi = v.astype(BF16)
    lo = (v - hi.astype(F32)).astype(BF16)
    return jnp.concatenate([hi, lo], axis=1)


def joined(v):
    return v[:, :128] + v[:, 128:]


def kernel(
    g_hbm, r_hbm, sel_hbm, cnt_hbm, upd_ref, nr_ref,
    sel_ref, cnt_ref, gv, rv, xsend, xrecv, idsend, idrecv, ysend, yrecv, zsend, zrecv, fin, gbuf,
    psem, gsem, rsem, xs, xr, ids_s, ids_r, ys, yr, zs, zr, as_, ar, near1, near2, near3,
):
    gi = lax.axis_index("grp")
    wi = lax.axis_index("wide")
    x, y = lax.rem(gi, NX), lax.div(gi, NX)
    z, c = lax.div(wi, NC), lax.rem(wi, NC)

    def dev(x_, y_, z_, c_):
        return (y_ * NX + x_, z_ * NC + c_)

    def mod(a, n):
        return lax.rem(a + n, n)

    picks = (
        pltpu.make_async_copy(sel_hbm, sel_ref, psem.at[0]),
        pltpu.make_async_copy(cnt_hbm, cnt_ref, psem.at[1]),
    )
    for cp in picks:
        cp.start()
    loads = []
    for j in range(CHUNKS):
        rows = pl.ds(32 * j, 32)
        a = pltpu.make_async_copy(g_hbm.at[0, 0, rows], gv.at[rows], gsem.at[j])
        b = pltpu.make_async_copy(r_hbm.at[0, 0, rows], rv.at[rows], rsem.at[j])
        a.start()
        b.start()
        loads.append((a, b))

    def signal(sem, x_, y_, z_, c_):
        pl.semaphore_signal(sem, inc=1, device_id=dev(x_, y_, z_, c_), device_id_type=MESH)

    barrier = pltpu.get_barrier_semaphore()
    for d in (1, NZ - 1):
        signal(barrier, x, y, mod(z + d, NZ), c)
    for d in (1, NY - 1):
        signal(barrier, x, mod(y + d, NY), z, c)
    for dx, dc in XC:
        signal(barrier, mod(x + dx, NX), y, z, mod(c + dc, NC))

    for cp in picks:
        cp.wait()
    sel = sel_ref[0, 0]
    eye = lax.broadcasted_iota(I32, (24, 24), 0) == lax.broadcasted_iota(I32, (24, 24), 1)
    used = jnp.sum(
        jnp.where(eye, jnp.broadcast_to(cnt_ref[0], (24, 24)).astype(F32), 0.0), axis=1, keepdims=True
    ).astype(I32)
    valid = lax.broadcasted_iota(I32, (24, 32), 1) < used
    low, high = jnp.bitwise_and(sel, 31), jnp.right_shift(sel, 5)
    target = jnp.where(valid, low * 4 + high, 512)
    odd = jnp.bitwise_and(lax.broadcasted_iota(I32, (24, 32), 0), 1)
    source = jnp.where(valid, low * 8 + high + 4 * odd, 512)
    target4 = jnp.concatenate([target] * 4, axis=1)
    source4 = jnp.concatenate([source] * 4, axis=1)
    for j in range(CHUNKS):
        for d in range(8):
            idsend[j, d] = target4[8 * j + d : 8 * j + d + 1]
    source_t = jnp.transpose(source4.astype(F32)).astype(I32)
    lane128 = lax.broadcasted_iota(I32, (1, 128), 1)
    lane256 = lax.broadcasted_iota(I32, (64, 256), 1)
    sub256 = lax.broadcasted_iota(I32, (256, 128), 0)
    ones = jnp.ones((128, 128), BF16)

    mine = 2 * x + c
    idcopies = []
    xcopies = []
    for j in range(CHUNKS):
        loads[j][0].wait()
        loads[j][1].wait()
        for p in range(4):
            s = 8 * j + 2 * p
            top = 32 * j + 8 * p
            blocks = []
            for q in range(32):
                lanes = slice(128 * q, 128 * (q + 1))
                blocks.append(gv[top : top + 8, lanes].astype(F32) + rv[top : top + 8, lanes])
            data = jnp.concatenate(blocks, axis=0)
            ids = jnp.concatenate(
                [
                    jnp.broadcast_to(source_t[:32, s : s + 1], (32, 256)),
                    jnp.broadcast_to(source_t[:32, s + 1 : s + 2], (32, 256)),
                ],
                axis=0,
            )
            pick = jnp.where(ids == lane256, 1.0, 0.0).astype(BF16)
            got = joined(jnp.dot(pick, halves(data), preferred_element_type=F32))
            xsend[j, 2 * p] = got[:32]
            xsend[j, 2 * p + 1] = got[32:]
            row = jnp.where(lane128 < 32, source4[s : s + 1], source4[s + 1 : s + 2])
            hit = jnp.where(jnp.broadcast_to(row, (256, 128)) == sub256, 1.0, 0.0).astype(BF16)
            mask = jnp.dot(hit, ones, preferred_element_type=F32)
            kept = jnp.where(mask > 0.5, 0.0, data)
            for q in range(32):
                nr_ref[0, 0, top : top + 8, 128 * q : 128 * (q + 1)] = kept[8 * q : 8 * q + 8]
        if j == 0:
            pl.semaphore_wait(barrier, 11)
            for d in (1, NZ - 1):
                signal(near1, x, y, mod(z + d, NZ), c)
            for d in (1, NY - 1):
                signal(near1, x, mod(y + d, NY), z, c)
            for n, (dx, dc) in enumerate(XC):
                tx, tc = mod(x + dx, NX), mod(c + dc, NC)
                cp = pltpu.make_async_remote_copy(
                    src_ref=idsend.at[:, 2 * tx + tc], dst_ref=idrecv.at[n + 1],
                    send_sem=ids_s.at[n], recv_sem=ids_r.at[n],
                    device_id=dev(tx, y, z, tc), device_id_type=MESH,
                )
                cp.start()
                idcopies.append(cp)
            idrecv[0] = idsend[:, mine]
        if j == 1:
            pl.semaphore_wait(near1, 4)
            for d in (2, NZ - 2):
                signal(near2, x, y, mod(z + d, NZ), c)
            for d in (2, NY - 2):
                signal(near2, x, mod(y + d, NY), z, c)
        copies = []
        for n, (dx, dc) in enumerate(XC):
            tx, tc = mod(x + dx, NX), mod(c + dc, NC)
            cp = pltpu.make_async_remote_copy(
                src_ref=xsend.at[j, 2 * tx + tc], dst_ref=xrecv.at[j, n + 1],
                send_sem=xs.at[j, n], recv_sem=xr.at[j, n],
                device_id=dev(tx, y, z, tc), device_id_type=MESH,
            )
            cp.start()
            copies.append(cp)
        xrecv[j, 0] = xsend[j, mine]
        xcopies.append(copies)

    pl.semaphore_wait(near2, 4)
    for d in (3, NZ - 3):
        signal(near3, x, y, mod(z + d, NZ), c)
    for cp in idcopies:
        cp.wait_recv()
    quarter = jnp.right_shift(lane128, 5)
    sub128 = lax.broadcasted_iota(I32, (128, 256), 0)
    ycopies = []
    for j in range(CHUNKS):
        for cp in xcopies[j]:
            cp.wait_recv()
        parts = []
        for h in range(2):
            row = idrecv[4 * h, j]
            for q in range(1, 4):
                row = jnp.where(quarter == q, idrecv[4 * h + q, j], row)
            parts.append(row)
        ids = jnp.broadcast_to(jnp.concatenate(parts, axis=1), (128, 256))
        put = jnp.where(ids == sub128, 1.0, 0.0).astype(BF16)
        arrived = xrecv[j].reshape(256, 128)
        ysend[j] = joined(jnp.dot(put, halves(arrived), preferred_element_type=F32)).reshape(8, 16, 128)
        copies = []
        for n, dy in enumerate(YS):
            ty = mod(y + dy, NY)
            cp = pltpu.make_async_remote_copy(
                src_ref=ysend.at[j, ty], dst_ref=yrecv.at[j, n],
                send_sem=ys.at[j, n], recv_sem=yr.at[j, n],
                device_id=dev(x, ty, z, c), device_id_type=MESH,
            )
            cp.start()
            copies.append(cp)
        ycopies.append(copies)

    pl.semaphore_wait(near3, 2)
    zx = lax.rem(z, NX)
    for j in range(CHUNKS):
        for cp in ycopies[j]:
            cp.wait_recv()
        total = ysend[j, y]
        for n in range(NY - 1):
            total = total + yrecv[j, n]
        zsend[j] = total
        tz = 4 * j + x

        def same_x(j=j, tz=tz):
            return pltpu.make_async_remote_copy(
                src_ref=zsend.at[j], dst_ref=zrecv.at[z],
                send_sem=zs.at[j], recv_sem=zr.at[z],
                device_id=dev(x, y, tz, c), device_id_type=MESH,
            )

        @pl.when(tz != z)
        def _():
            same_x().start()

        @pl.when(tz == z)
        def _():
            zrecv[z] = zsend[j]

    owner = zx == x

    @pl.when(owner)
    def _():
        for s in range(NZ):
            @pl.when(z != s)
            def _():
                pltpu.make_async_remote_copy(
                    src_ref=zsend.at[0], dst_ref=zrecv.at[s],
                    send_sem=zs.at[0], recv_sem=zr.at[s],
                    device_id=dev(x, y, z, 1 - c), device_id_type=MESH,
                ).wait_recv()

        result = zrecv[0]
        for s in range(1, NZ):
            result = result + zrecv[s]
        result = result * (1.0 / 32.0)
        fin[...] = result
        for n, (dx, dy) in enumerate(GS):
            pltpu.make_async_remote_copy(
                src_ref=fin, dst_ref=gbuf.at[y],
                send_sem=as_.at[n], recv_sem=ar.at[y],
                device_id=dev(mod(x + dx, NX), mod(y + dy, NY), z, c), device_id_type=MESH,
            ).start()
        gbuf[y] = result

    for cp in idcopies:
        cp.wait_send()
    for copies in xcopies + ycopies:
        for cp in copies:
            cp.wait_send()
    for j in range(CHUNKS):
        tz = 4 * j + x

        @pl.when(tz != z)
        def _():
            pltpu.make_async_remote_copy(
                src_ref=zsend.at[j], dst_ref=zrecv.at[z],
                send_sem=zs.at[j], recv_sem=zr.at[z],
                device_id=dev(x, y, tz, c), device_id_type=MESH,
            ).wait_send()
    for s in range(NY):
        @pl.when(jnp.logical_or(zx != x, y != s))
        def _():
            pltpu.make_async_remote_copy(
                src_ref=fin, dst_ref=gbuf.at[s],
                send_sem=as_.at[0], recv_sem=ar.at[s],
                device_id=dev(x, y, z, 1 - c), device_id_type=MESH,
            ).wait_recv()

    @pl.when(owner)
    def _():
        for n, (dx, dy) in enumerate(GS):
            pltpu.make_async_remote_copy(
                src_ref=fin, dst_ref=gbuf.at[y],
                send_sem=as_.at[n], recv_sem=ar.at[y],
                device_id=dev(mod(x + dx, NX), mod(y + dy, NY), z, c), device_id_type=MESH,
            ).wait_send()

    for p in range(32):
        upd_ref[0, :, 128 * p : 128 * (p + 1)] = gbuf[p // 4, 4 * (p % 4) : 4 * (p % 4) + 4]


def flush(upd_ref, nr_ref, upd_hbm, nr_hbm, sem):
    copies = [pltpu.make_async_copy(upd_ref, upd_hbm, sem.at[4])]
    for n in range(4):
        rows = pl.ds(24 * n, 24)
        copies.append(pltpu.make_async_copy(nr_ref.at[0, 0, rows], nr_hbm.at[0, 0, rows], sem.at[n]))
    for cp in copies:
        cp.start()
    for cp in copies:
        cp.wait()


def body(gradient, residual, selected, counts):
    dma = pltpu.SemaphoreType.DMA
    plain = pltpu.SemaphoreType.REGULAR
    vmem = pl.BlockSpec(memory_space=pltpu.VMEM)
    hbm = pl.BlockSpec(memory_space=pltpu.HBM)
    update, rest = pl.pallas_call(
        kernel,
        name="owner_sums",
        out_shape=(
            pltpu.VMEM((1, 4, 4096), F32),
            pltpu.VMEM((1, 1, 96, 4096), F32),
        ),
        in_specs=[hbm, hbm, hbm, hbm],
        out_specs=(vmem, vmem),
        scratch_shapes=[
            pltpu.VMEM((1, 1, 24, 32), I32),
            pltpu.VMEM((1, 1, 24), I32),
            pltpu.VMEM((96, 4096), BF16),
            pltpu.VMEM((96, 4096), F32),
            pltpu.VMEM((CHUNKS, 8, 32, 128), F32),
            pltpu.VMEM((CHUNKS, 8, 32, 128), F32),
            pltpu.VMEM((CHUNKS, 8, 1, 128), I32),
            pltpu.VMEM((8, CHUNKS, 1, 128), I32),
            pltpu.VMEM((CHUNKS, 8, 16, 128), F32),
            pltpu.VMEM((CHUNKS, 7, 16, 128), F32),
            pltpu.VMEM((CHUNKS, 16, 128), F32),
            pltpu.VMEM((NZ, 16, 128), F32),
            pltpu.VMEM((16, 128), F32),
            pltpu.VMEM((NY, 16, 128), F32),
            dma((2,)), dma((CHUNKS,)), dma((CHUNKS,)),
            dma((CHUNKS, 7)), dma((CHUNKS, 7)),
            dma((7,)), dma((7,)),
            dma((CHUNKS, 7)), dma((CHUNKS, 7)),
            dma((CHUNKS,)), dma((NZ,)),
            dma((31,)), dma((NY,)),
            plain, plain, plain,
        ],
        compiler_params=pltpu.CompilerParams(collective_id=0, has_side_effects=True, vmem_limit_bytes=62 << 20),
    )(gradient, residual, selected, counts)
    return pl.pallas_call(
        flush,
        name="write_results",
        out_shape=(
            jax.ShapeDtypeStruct((1, 4, 4096), F32),
            jax.ShapeDtypeStruct((1, 1, 96, 4096), F32),
        ),
        in_specs=[vmem, vmem],
        out_specs=(hbm, hbm),
        scratch_shapes=[dma((5,))],
        compiler_params=pltpu.CompilerParams(vmem_limit_bytes=1 << 20),
    )(update, rest)


def solution(mesh):
    return jax.shard_map(
        body,
        mesh=mesh,
        in_specs=(
            P("grp", "wide", None, None),
            P("grp", "wide", None, None),
            P("grp", "wide", None, None),
            P("grp", "wide", None),
        ),
        out_specs=(P("wide", None, None), P("grp", "wide", None, None)),
        check_vma=False,
    )
```

```python
import jax
import jax.numpy as jnp
from jax import lax
from jax.experimental import pallas as pl
from jax.experimental.pallas import tpu as pltpu
from jax.sharding import PartitionSpec as P

MESH = pl.DeviceIdType.MESH
NX, NY, NZ, NC = 4, 8, 12, 2
CHUNKS = 3
F32, BF16, I32 = jnp.float32, jnp.bfloat16, jnp.int32


def ring(d, n):
    return min(d % n, (-d) % n)


XC = sorted(
    [(dx, dc) for dx in range(NX) for dc in range(NC) if dx or dc],
    key=lambda o: -(2 * ring(o[0], NX) + o[1]),
)
YS = sorted(range(1, NY), key=lambda d: -ring(d, NY))
GS = sorted(
    [(dx, dy) for dx in range(NX) for dy in range(NY) if dx or dy],
    key=lambda o: -(ring(o[0], NX) + ring(o[1], NY)),
)


def halves(v):
    hi = v.astype(BF16)
    lo = (v - hi.astype(F32)).astype(BF16)
    return jnp.concatenate([hi, lo], axis=1)


def joined(v):
    return v[:, :128] + v[:, 128:]


def kernel(
    g_hbm, r_hbm, sel_hbm, cnt_hbm, upd_ref, nr_ref,
    sel_ref, cnt_ref, gv, rv, xsend, xrecv, idsend, idrecv, ysend, yrecv, zsend, zrecv, fin, gbuf,
    psem, gsem, rsem, xs, xr, ids_s, ids_r, ys, yr, zs, zr, as_, ar, near1, near2, near3,
):
    gi = lax.axis_index("grp")
    wi = lax.axis_index("wide")
    x, y = lax.rem(gi, NX), lax.div(gi, NX)
    z, c = lax.div(wi, NC), lax.rem(wi, NC)

    def dev(x_, y_, z_, c_):
        return (y_ * NX + x_, z_ * NC + c_)

    def mod(a, n):
        return lax.rem(a + n, n)

    def signal(sem, x_, y_, z_, c_):
        pl.semaphore_signal(sem, inc=1, device_id=dev(x_, y_, z_, c_), device_id_type=MESH)

    barrier = pltpu.get_barrier_semaphore()
    for d in (1, NZ - 1):
        signal(barrier, x, y, mod(z + d, NZ), c)
    for d in (1, NY - 1):
        signal(barrier, x, mod(y + d, NY), z, c)
    for dx, dc in XC:
        signal(barrier, mod(x + dx, NX), y, z, mod(c + dc, NC))

    picks = (
        pltpu.make_async_copy(sel_hbm, sel_ref, psem.at[0]),
        pltpu.make_async_copy(cnt_hbm, cnt_ref, psem.at[1]),
    )
    for cp in picks:
        cp.start()
    loads = []
    for j in range(CHUNKS):
        rows = pl.ds(32 * j, 32)
        a = pltpu.make_async_copy(g_hbm.at[0, 0, rows], gv.at[rows], gsem.at[j])
        b = pltpu.make_async_copy(r_hbm.at[0, 0, rows], rv.at[rows], rsem.at[j])
        a.start()
        b.start()
        loads.append((a, b))

    for cp in picks:
        cp.wait()
    sel = sel_ref[0, 0]
    eye = lax.broadcasted_iota(I32, (24, 24), 0) == lax.broadcasted_iota(I32, (24, 24), 1)
    used = jnp.sum(
        jnp.where(eye, jnp.broadcast_to(cnt_ref[0], (24, 24)).astype(F32), 0.0), axis=1, keepdims=True
    ).astype(I32)
    valid = lax.broadcasted_iota(I32, (24, 32), 1) < used
    low, high = jnp.bitwise_and(sel, 31), jnp.right_shift(sel, 5)
    target = jnp.where(valid, low * 4 + high, 512)
    odd = jnp.bitwise_and(lax.broadcasted_iota(I32, (24, 32), 0), 1)
    source = jnp.where(valid, low * 8 + high + 4 * odd, 512)
    target4 = jnp.concatenate([target] * 4, axis=1)
    source4 = jnp.concatenate([source] * 4, axis=1)
    for j in range(CHUNKS):
        for d in range(8):
            idsend[d, j] = target4[8 * j + d : 8 * j + d + 1]
    source_t = jnp.transpose(source4.astype(F32)).astype(I32)
    lane128 = lax.broadcasted_iota(I32, (1, 128), 1)
    lane256 = lax.broadcasted_iota(I32, (64, 256), 1)
    sub256 = lax.broadcasted_iota(I32, (256, 128), 0)
    ones = jnp.ones((128, 128), BF16)

    def accumulated(top):
        rows = []
        for q in range(32):
            lanes = slice(128 * q, 128 * (q + 1))
            rows.append(gv[top : top + 8, lanes].astype(F32) + rv[top : top + 8, lanes])
        return jnp.concatenate(rows, axis=0)

    mine = 2 * x + c
    idcopies = []
    xcopies = []
    for j in range(CHUNKS):
        loads[j][0].wait()
        loads[j][1].wait()
        for p in range(4):
            s = 8 * j + 2 * p
            top = 32 * j + 8 * p
            data = accumulated(top)
            ids = jnp.concatenate(
                [
                    jnp.broadcast_to(source_t[:32, s : s + 1], (32, 256)),
                    jnp.broadcast_to(source_t[:32, s + 1 : s + 2], (32, 256)),
                ],
                axis=0,
            )
            pick = jnp.where(ids == lane256, 1.0, 0.0).astype(BF16)
            got = joined(jnp.dot(pick, halves(data), preferred_element_type=F32))
            xsend[j, 2 * p] = got[:32]
            xsend[j, 2 * p + 1] = got[32:]
        if j == 0:
            pl.semaphore_wait(barrier, 11)
            for d in (1, NZ - 1):
                signal(near1, x, y, mod(z + d, NZ), c)
            for d in (1, NY - 1):
                signal(near1, x, mod(y + d, NY), z, c)
            for n, (dx, dc) in enumerate(XC):
                tx, tc = mod(x + dx, NX), mod(c + dc, NC)
                cp = pltpu.make_async_remote_copy(
                    src_ref=idsend.at[2 * tx + tc], dst_ref=idrecv.at[n + 1],
                    send_sem=ids_s.at[n], recv_sem=ids_r.at[n],
                    device_id=dev(tx, y, z, tc), device_id_type=MESH,
                )
                cp.start()
                idcopies.append(cp)
            idrecv[0] = idsend[mine]
        if j == 1:
            pl.semaphore_wait(near1, 4)
            for d in (2, NZ - 2):
                signal(near2, x, y, mod(z + d, NZ), c)
            for d in (2, NY - 2):
                signal(near2, x, mod(y + d, NY), z, c)
        copies = []
        for n, (dx, dc) in enumerate(XC):
            tx, tc = mod(x + dx, NX), mod(c + dc, NC)
            cp = pltpu.make_async_remote_copy(
                src_ref=xsend.at[j, 2 * tx + tc], dst_ref=xrecv.at[j, n + 1],
                send_sem=xs.at[j, n], recv_sem=xr.at[j, n],
                device_id=dev(tx, y, z, tc), device_id_type=MESH,
            )
            cp.start()
            copies.append(cp)
        xrecv[j, 0] = xsend[j, mine]
        xcopies.append(copies)
        for p in range(4 * j, 4 * j + 4):
            s, top = 2 * p, 8 * p
            row = jnp.where(lane128 < 32, source4[s : s + 1], source4[s + 1 : s + 2])
            hit = jnp.where(jnp.broadcast_to(row, (256, 128)) == sub256, 1.0, 0.0).astype(BF16)
            mask = jnp.dot(hit, ones, preferred_element_type=F32)
            kept = jnp.where(mask > 0.5, 0.0, accumulated(top))
            for q in range(32):
                nr_ref[0, 0, top : top + 8, 128 * q : 128 * (q + 1)] = kept[8 * q : 8 * q + 8]

    pl.semaphore_wait(near2, 4)
    for d in (3, NZ - 3):
        signal(near3, x, y, mod(z + d, NZ), c)
    for cp in idcopies:
        cp.wait_recv()
    quarter = jnp.right_shift(lane128, 5)
    sub128 = lax.broadcasted_iota(I32, (128, 256), 0)
    ycopies = []
    for j in range(CHUNKS):
        for cp in xcopies[j]:
            cp.wait_recv()
        parts = []
        for h in range(2):
            row = idrecv[4 * h, j]
            for q in range(1, 4):
                row = jnp.where(quarter == q, idrecv[4 * h + q, j], row)
            parts.append(row)
        ids = jnp.broadcast_to(jnp.concatenate(parts, axis=1), (128, 256))
        put = jnp.where(ids == sub128, 1.0, 0.0).astype(BF16)
        arrived = xrecv[j].reshape(256, 128)
        ysend[j] = joined(jnp.dot(put, halves(arrived), preferred_element_type=F32)).reshape(8, 16, 128)
        copies = []
        for n, dy in enumerate(YS):
            ty = mod(y + dy, NY)
            cp = pltpu.make_async_remote_copy(
                src_ref=ysend.at[j, ty], dst_ref=yrecv.at[j, n],
                send_sem=ys.at[j, n], recv_sem=yr.at[j, n],
                device_id=dev(x, ty, z, c), device_id_type=MESH,
            )
            cp.start()
            copies.append(cp)
        ycopies.append(copies)

    pl.semaphore_wait(near3, 2)
    zx = lax.rem(z, NX)

    def z_copy(j, h):
        return pltpu.make_async_remote_copy(
            src_ref=zsend.at[j, h], dst_ref=zrecv.at[z],
            send_sem=zs.at[j, h], recv_sem=zr.at[z],
            device_id=dev(mod(x + h, NX), y, 4 * j + x, c), device_id_type=MESH,
        )

    second = mod(zx + 1, NX) == x
    half = mod(x - zx, NX)

    def g_copy(n, dx, dy):
        return pltpu.make_async_remote_copy(
            src_ref=fin, dst_ref=gbuf.at[y, half],
            send_sem=as_.at[n], recv_sem=ar.at[y, half],
            device_id=dev(mod(x + dx, NX), mod(y + dy, NY), z, c), device_id_type=MESH,
        )

    for j in range(CHUNKS):
        for cp in ycopies[j]:
            cp.wait_recv()
        total = ysend[j, y]
        for n in range(NY - 1):
            total = total + yrecv[j, n]
        zsend[j, 0] = total[:8]
        zsend[j, 1] = total[8:]
        tz = 4 * j + x
        z_copy(j, 1).start()

        @pl.when(tz != z)
        def _(j=j):
            z_copy(j, 0).start()

        @pl.when(tz == z)
        def _(total=total):
            zrecv[z] = total[:8]

    owner = jnp.logical_or(zx == x, second)

    @pl.when(owner)
    def _():
        for s in range(NZ):
            @pl.when(jnp.logical_or(z != s, second))
            def _():
                pltpu.make_async_remote_copy(
                    src_ref=zsend.at[0, 0], dst_ref=zrecv.at[s],
                    send_sem=zs.at[0, 0], recv_sem=zr.at[s],
                    device_id=dev(x, y, z, 1 - c), device_id_type=MESH,
                ).wait_recv()

        result = zrecv[0]
        for s in range(1, NZ):
            result = result + zrecv[s]
        result = result * (1.0 / 32.0)
        fin[...] = result
        for n, (dx, dy) in enumerate(GS):
            g_copy(n, dx, dy).start()
        gbuf[y, half] = result

    for cp in idcopies:
        cp.wait_send()
    for copies in xcopies + ycopies:
        for cp in copies:
            cp.wait_send()
    for j in range(CHUNKS):
        z_copy(j, 1).wait_send()

        @pl.when(4 * j + x != z)
        def _(j=j):
            z_copy(j, 0).wait_send()
    for s in range(NY):
        for h in range(2):
            @pl.when(jnp.logical_or(mod(zx + h, NX) != x, y != s))
            def _(s=s, h=h):
                pltpu.make_async_remote_copy(
                    src_ref=fin, dst_ref=gbuf.at[s, h],
                    send_sem=as_.at[0], recv_sem=ar.at[s, h],
                    device_id=dev(x, y, z, 1 - c), device_id_type=MESH,
                ).wait_recv()

    @pl.when(owner)
    def _():
        for n, (dx, dy) in enumerate(GS):
            g_copy(n, dx, dy).wait_send()

    for p in range(32):
        upd_ref[0, :, 128 * p : 128 * (p + 1)] = gbuf[p // 4, p // 2 % 2, 4 * (p % 2) : 4 * (p % 2) + 4]


def flush(upd_ref, nr_ref, upd_hbm, nr_hbm, sem):
    copies = [pltpu.make_async_copy(upd_ref, upd_hbm, sem.at[4])]
    for n in range(4):
        rows = pl.ds(24 * n, 24)
        copies.append(pltpu.make_async_copy(nr_ref.at[0, 0, rows], nr_hbm.at[0, 0, rows], sem.at[n]))
    for cp in copies:
        cp.start()
    for cp in copies:
        cp.wait()


def body(gradient, residual, selected, counts):
    dma = pltpu.SemaphoreType.DMA
    plain = pltpu.SemaphoreType.REGULAR
    vmem = pl.BlockSpec(memory_space=pltpu.VMEM)
    hbm = pl.BlockSpec(memory_space=pltpu.HBM)
    update, rest = pl.pallas_call(
        kernel,
        name="owner_sums",
        out_shape=(
            pltpu.VMEM((1, 4, 4096), F32),
            pltpu.VMEM((1, 1, 96, 4096), F32),
        ),
        in_specs=[hbm, hbm, hbm, hbm],
        out_specs=(vmem, vmem),
        scratch_shapes=[
            pltpu.VMEM((1, 1, 24, 32), I32),
            pltpu.VMEM((1, 1, 24), I32),
            pltpu.VMEM((96, 4096), BF16),
            pltpu.VMEM((96, 4096), F32),
            pltpu.VMEM((CHUNKS, 8, 32, 128), F32),
            pltpu.VMEM((CHUNKS, 8, 32, 128), F32),
            pltpu.VMEM((8, CHUNKS, 1, 128), I32),
            pltpu.VMEM((8, CHUNKS, 1, 128), I32),
            pltpu.VMEM((CHUNKS, 8, 16, 128), F32),
            pltpu.VMEM((CHUNKS, 7, 16, 128), F32),
            pltpu.VMEM((CHUNKS, 2, 8, 128), F32),
            pltpu.VMEM((NZ, 8, 128), F32),
            pltpu.VMEM((8, 128), F32),
            pltpu.VMEM((NY, 2, 8, 128), F32),
            dma((2,)), dma((CHUNKS,)), dma((CHUNKS,)),
            dma((CHUNKS, 7)), dma((CHUNKS, 7)),
            dma((7,)), dma((7,)),
            dma((CHUNKS, 7)), dma((CHUNKS, 7)),
            dma((CHUNKS, 2)), dma((NZ,)),
            dma((31,)), dma((NY, 2)),
            plain, plain, plain,
        ],
        compiler_params=pltpu.CompilerParams(collective_id=0, has_side_effects=True, vmem_limit_bytes=62 << 20),
    )(gradient, residual, selected, counts)
    return pl.pallas_call(
        flush,
        name="write_results",
        out_shape=(
            jax.ShapeDtypeStruct((1, 4, 4096), F32),
            jax.ShapeDtypeStruct((1, 1, 96, 4096), F32),
        ),
        in_specs=[vmem, vmem],
        out_specs=(hbm, hbm),
        scratch_shapes=[dma((5,))],
        compiler_params=pltpu.CompilerParams(vmem_limit_bytes=1 << 20),
    )(update, rest)


def solution(mesh):
    return jax.shard_map(
        body,
        mesh=mesh,
        in_specs=(
            P("grp", "wide", None, None),
            P("grp", "wide", None, None),
            P("grp", "wide", None, None),
            P("grp", "wide", None),
        ),
        out_specs=(P("wide", None, None), P("grp", "wide", None, None)),
        check_vma=False,
    )
```
